256 devices in a mesh: sx: 8 (over y, core), sy: 4 (over x), sz: 8 (over z).
Axes of the slice: x: 4, y: 4, z: 8, core: 2. Of those that a mesh axis runs over, the one named last changes fastest.
Arguments:
- right_side: bfloat16 [8, 4, 8, 1536, 256], P('sx', 'sy', 'sz'), may hold values from -6 to 6
- interface_inverse: bfloat16 [8, 4, 8, 1536, 1536], P('sx', 'sy', 'sz'), may hold values from -2 to 2, as said below
- face_link: int32 [8, 4, 8, 4], P('sx', 'sy', 'sz'), may hold values 0 or 1
- far_target: int32 [8, 4, 8, 64, 1], P('sx', 'sy', 'sz'), may hold values from 0 to 63; in each aligned block of 64 rows (0 to 63, 64 to 127, ..., all dimensions but the last counted through in order) at most 3 rows name the same one
- far_rank: int32 [8, 4, 8, 64], P('sx', 'sy', 'sz'), may hold values from 1 to 16
- far_basis: bfloat16 [8, 4, 8, 64, 16, 1536], P('sx', 'sy', 'sz'), may hold values from -0.15625 to 0.15625
- patch_basis: bfloat16 [8, 4, 8, 16, 1536], P('sx', 'sy', 'sz'), may hold values from -0.1875 to 0.1875
- corner_basis: bfloat16 [8, 4, 8, 8, 1536], P('sx', 'sy', 'sz'), may hold values from -1 to 1
- corner_row: int32 [8, 4, 8, 8], P('sx', 'sy', 'sz'), may hold values from 0 to 2047
- coarse_inverse: bfloat16 [2048, 2048], P('sy'), may hold values from -2 to 2, as said below
Outputs:
- multipliers: float32 [8, 4, 8, 1536, 256], P('sx', 'sy', 'sz')
- interface_field: bfloat16 [8, 4, 8, 1536, 256], P('sx', 'sy', 'sz')
The draws below stay inside these ranges and needn't reach their ends.
Inputs may be any that keep to these rules, and one draw needn't show every extreme that they name: `far_target`: within one subdomain's 64 entries no target is named more than 3 times, a bound that some block reaches. `interface_inverse`: each subdomain's block is a dense matrix with a positive diagonal that exceeds its row's off-diagonal magnitude in the root-mean-square sense. `coarse_inverse`: A dense matrix with a positive diagonal that exceeds its row's off-diagonal magnitude in the root-mean-square sense.
All inputs are finite; a program needn't handle non-finite values. No bound on the sum of `face_link` on one device may be relied on, other than what follows from the above.
Results may differ from the reference program's by a relative error of at most 0.0085.
Values may be sent and summed in bfloat16 or wider, within the bound.
No kernel may reach another device: no remote copies, remote signals or barrier semaphores. Data moves between devices by JAX's collectives and lax.ppermute only.
A program may use at most 64 MiB of HBM per device.

```python
import math
import jax
import jax.numpy as jnp
import numpy as np
from jax import lax

IF = 1536
NRHS = 256
RMAX = 16
CORNERS = 8
MOST = 3
ITERS = 2
GROUP = 64
FAR = 64
NC = 2048
N_SX = 8
N_SY = 4
N_SZ = 8


def draw_interface_inverse(key, part):
    noise_key = jax.random.fold_in(key, 11)
    diagonal_key = jax.random.fold_in(key, 12)
    shape = (N_SX, N_SY, N_SZ, IF, IF)
    noise = jax.random.truncated_normal(noise_key, -4.0, 4.0, shape, jnp.float32)
    diagonal = jax.random.uniform(diagonal_key, (N_SX, N_SY, N_SZ, IF), jnp.float32, 0.3, 0.9)
    scaled = noise * (0.4 / jnp.sqrt(jnp.float32(IF)))
    return (scaled + diagonal[..., None] * jnp.eye(IF, dtype=jnp.float32)).astype(jnp.bfloat16)


def draw_coarse_inverse(key, part):
    noise_key = jax.random.fold_in(key, 21)
    diagonal_key = jax.random.fold_in(key, 22)
    noise = jax.random.truncated_normal(noise_key, -4.0, 4.0, (NC, NC), jnp.float32)
    diagonal = jax.random.uniform(diagonal_key, (NC,), jnp.float32, 0.3, 0.9)
    scaled = noise * (0.4 / jnp.sqrt(jnp.float32(NC)))
    return (scaled + diagonal[:, None] * jnp.eye(NC, dtype=jnp.float32)).astype(jnp.bfloat16)


def plant(values, rng, low, largest):
    longest = values.shape.index(max(values.shape))
    spots = []
    for shift in (0, 1):
        where = [jax.random.randint(jax.random.fold_in(rng, axis), (), 0, length) for axis, length in enumerate(values.shape)]
        where[longest] = (where[longest] + shift) % values.shape[longest]
        spots.append(tuple(where))
    return values.at[spots[0]].set(low).at[spots[1]].set(largest)


def shard_levels(own_key, shape, cuts, smallest, high):
    factor_of = 1.0
    for position, shards_of in cuts:
        draws = jax.random.uniform(jax.random.fold_in(jax.random.fold_in(own_key, 6), position), (shards_of,), jnp.float32, smallest / len(cuts), high / len(cuts))
        factor_of = factor_of * jnp.repeat(jnp.exp(draws), shape[position] // shards_of).reshape((-1,) + (1,) * (len(shape) - 1 - position))
    return factor_of


def shared_out(own_key, own, number, rows, number_of, top, most, lean):
    ranking = jax.random.permutation(own_key, number_of)
    heavy_load, common = portions_of(number_of, rows * top, most, lean, True), portions_of(number_of, rows * top, most, lean, False)
    places = jnp.arange(number_of)

    def named(sizes, turn):
        used = int((sizes > 0).sum())
        fixed = max(1, used // 4)
        shifted = fixed + (places - fixed + turn * (used - fixed)) % max(1, number_of - fixed)
        return jnp.zeros((number_of,), jnp.int32).at[ranking[jnp.where(places < fixed, places, shifted)]].set(jnp.asarray(sizes, jnp.int32))

    sizes = jnp.where(number % 4 == 0, named(heavy_load, number // 4), named(common, number - number // 4 - 1))
    mixed = jax.random.permutation(jax.random.fold_in(own, 3), number_of)
    donor, receiver = mixed[0:number_of // 2 * 2:2], mixed[1:number_of // 2 * 2:2]
    slack = jnp.minimum(sizes[donor] - 1, most - sizes[receiver]) // 2
    slack = jnp.where((donor == ranking[0]) | (receiver == ranking[0]) | (sizes[receiver] == 0), 0, jnp.maximum(slack, 0))
    shifted = jax.random.randint(jax.random.fold_in(own, 4), (number_of // 2,), 0, 1 << 20) % (slack + 1)
    sizes = sizes.at[donor].add(-shifted).at[receiver].add(shifted)
    members = jnp.searchsorted(jnp.cumsum(sizes), jnp.arange(rows * top), side="right").astype(jnp.int32)
    grid = members.reshape(top, rows).T
    grid = grid[jax.random.permutation(jax.random.fold_in(own, 1), rows)]
    turn = jax.random.randint(jax.random.fold_in(own, 2), (rows, 1), 0, top)
    return jnp.take_along_axis(grid, (jnp.arange(top)[None, :] + turn) % top, axis=1)


def portions_of(number_of, total, bound, slope, full):
    weights = [(1 << 20) // math.isqrt(rank ** slope) + 1 for rank in range(1, number_of + 1)]
    largest = bound if full else min(bound, max(-(-total // number_of), total * weights[0] // sum(weights)))
    least = 1 if total - largest >= number_of - 1 else 0
    given, spare = [largest] + [least] * (number_of - 1), total - largest - least * (number_of - 1)
    while spare > 0:
        candidates = [i for i in range(1, number_of) if given[i] < largest] or [i for i in range(1, number_of) if given[i] < bound]
        whole, budget = sum([weights[i] for i in candidates]), spare
        for i in candidates:
            more = min(bound - given[i], max(1, budget * weights[i] // whole), spare)
            given[i] = given[i] + more
            spare = spare - more
    return np.array(given)


def gaussian(own_key, dims, deviation, reach, shards=(), kind=jnp.bfloat16):
    values = deviation * jax.random.normal(own_key, dims, jnp.float32)
    if shards:
        values = values * shard_levels(own_key, dims, shards, -0.22, 0.18)
    return jnp.clip(values, -reach, reach).astype(kind)


def setup_inputs(seed: int = 0) -> dict:
    keys = jax.random.split(jax.random.key(seed), 11)
    right_side = gaussian(keys[0], (N_SX, N_SY, N_SZ, IF, NRHS), 1.0, 6.0, ((0, 8), (1, 4), (2, 8)))
    interface_inverse = draw_interface_inverse(jax.random.fold_in(keys[10], 71), 0)
    face_link = plant((jax.random.randint(keys[2], (N_SX, N_SY, N_SZ, 4), 0, 4) < 3).astype(jnp.int32), jax.random.fold_in(keys[2], 1), 0, 1)
    far_target_keys = jax.random.split(jax.random.fold_in(keys[3], 1), N_SX * N_SY * N_SZ * FAR // FAR)
    far_target_turns = jax.random.permutation(jax.random.fold_in(keys[3], 3), N_SX * N_SY * N_SZ * FAR // FAR)
    far_target = jax.vmap(lambda own, number: shared_out(jax.random.fold_in(keys[3], 2), own, number, FAR, GROUP, 1, MOST, 2))(far_target_keys, far_target_turns).reshape((N_SX, N_SY, N_SZ, FAR, 1))
    far_rank = plant(jax.random.randint(keys[4], (N_SX, N_SY, N_SZ, FAR), 1, RMAX + 1), jax.random.fold_in(keys[4], 1), 1, RMAX).astype(jnp.int32)
    far_basis = gaussian(keys[5], (N_SX, N_SY, N_SZ, FAR, RMAX, IF), IF ** -0.5, 0.15625, ((0, 8), (1, 4), (2, 8)))
    patch_basis = gaussian(keys[6], (N_SX, N_SY, N_SZ, RMAX, IF), (RMAX * FAR) ** -0.5, 0.1875, ((0, 8), (1, 4), (2, 8)))
    corner_basis = gaussian(keys[7], (N_SX, N_SY, N_SZ, CORNERS, IF), 0.16, 1.0, ((0, 8), (1, 4), (2, 8)))
    corner_row = plant(jax.random.randint(keys[8], (N_SX, N_SY, N_SZ, CORNERS), 0, NC), jax.random.fold_in(keys[8], 1), 0, NC - 1).astype(jnp.int32)
    coarse_inverse = draw_coarse_inverse(jax.random.fold_in(keys[10], 71), 0)
    return dict(right_side=right_side, interface_inverse=interface_inverse, face_link=face_link, far_target=far_target, far_rank=far_rank, far_basis=far_basis, patch_basis=patch_basis, corner_basis=corner_basis, corner_row=corner_row, coarse_inverse=coarse_inverse)


def solve_each(interface_inverse, multipliers):
    order_size = interface_inverse.shape[-1]
    flat_inverse = interface_inverse.reshape(-1, order_size, order_size)
    flat_values = multipliers.astype(jnp.bfloat16).reshape((-1,) + multipliers.shape[-2:])

    def solve_one(pair):
        return jnp.dot(pair[0].astype(jnp.float32), pair[1].astype(jnp.float32), preferred_element_type=jnp.float32).astype(jnp.bfloat16)

    return lax.map(solve_one, (flat_inverse, flat_values)).reshape(multipliers.shape)


def far_coefficients(far_basis, solved, far_rank):
    flat_basis = far_basis.reshape((-1,) + far_basis.shape[-3:])
    flat_solved = solved.reshape((-1,) + solved.shape[-2:])
    flat_rank = far_rank.reshape(-1, far_rank.shape[-1])

    def coefficient_one(triple):
        basis, values, ranks = triple
        product = jnp.einsum('eri,in->ern', basis.astype(jnp.float32), values.astype(jnp.float32))
        kept = (jnp.arange(basis.shape[1], dtype=jnp.int32)[None, :] < ranks[:, None]).astype(jnp.float32)
        return (product * kept[:, :, None]).astype(jnp.bfloat16)

    result = lax.map(coefficient_one, (flat_basis, flat_solved, flat_rank))
    return result.reshape(far_basis.shape[:4] + (far_basis.shape[4], solved.shape[-1]))


def neighbour_faces(solved, face_link):
    face_rows = IF // 6
    values = solved.astype(jnp.float32)
    links = face_link.astype(jnp.float32)
    face_zero = values[..., 0:face_rows, :]
    face_one = values[..., face_rows:2 * face_rows, :]
    face_two = values[..., 2 * face_rows:3 * face_rows, :]
    face_three = values[..., 3 * face_rows:4 * face_rows, :]
    from_lower_x = jnp.concatenate([jnp.zeros_like(face_one[:1]), face_one[:-1]], axis=0)
    from_upper_x = jnp.concatenate([face_zero[1:], jnp.zeros_like(face_zero[:1])], axis=0)
    from_lower_y = jnp.concatenate([jnp.zeros_like(face_three[:, :1]), face_three[:, :-1]], axis=1)
    from_upper_y = jnp.concatenate([face_two[:, 1:], jnp.zeros_like(face_two[:, :1])], axis=1)
    rest = jnp.zeros(values.shape[:-2] + (IF - 4 * face_rows, values.shape[-1]), jnp.float32)
    return jnp.concatenate([
        links[..., 0, None, None] * from_lower_x,
        links[..., 1, None, None] * from_upper_x,
        links[..., 2, None, None] * from_lower_y,
        links[..., 3, None, None] * from_upper_y,
        rest], axis=-2)


def reference(right_side, interface_inverse, face_link, far_target, far_rank, far_basis, patch_basis, corner_basis, corner_row, coarse_inverse):
    source = right_side.astype(jnp.float32)
    multipliers = source
    target_hot = (far_target[..., 0][..., None] == jnp.arange(GROUP, dtype=jnp.int32)).astype(jnp.float32)
    for sweep in range(ITERS):
        solved = solve_each(interface_inverse, multipliers)
        neighbour = neighbour_faces(solved, face_link)
        coefficient = far_coefficients(far_basis, solved, far_rank)
        arrived = jnp.einsum('xyzeg,xyzern->ygrn', target_hot, coefficient.astype(jnp.float32))
        arrived = arrived.reshape(N_SY, N_SX, N_SZ, RMAX, NRHS).transpose(1, 0, 2, 3, 4)
        arrived_rounded = arrived.astype(jnp.bfloat16)
        far_term = jnp.einsum('xyzri,xyzrn->xyzin', patch_basis.astype(jnp.float32), arrived_rounded.astype(jnp.float32))
        corner_terms = jnp.einsum('xyzci,xyzin->xyzcn', corner_basis.astype(jnp.float32), solved.astype(jnp.float32))
        coarse_sum = jax.ops.segment_sum(corner_terms.reshape(-1, NRHS), corner_row.reshape(-1), num_segments=NC).astype(jnp.bfloat16)
        coarse_field = jnp.dot(coarse_inverse, coarse_sum, preferred_element_type=jnp.float32).astype(jnp.bfloat16)
        picked = coarse_field[corner_row]
        correction = jnp.einsum('xyzci,xyzcn->xyzin', corner_basis.astype(jnp.float32), picked.astype(jnp.float32))
        multipliers = multipliers + source - (solved.astype(jnp.float32) - neighbour) - far_term - correction
    interface_field = solve_each(interface_inverse, multipliers)
    return multipliers, interface_field
```

```python
import jax
import jax.numpy as jnp
from jax import lax
from jax.sharding import Mesh
from jax.sharding import PartitionSpec as P

ITERS = 2
RADIX = 64
GRID = ("y", "core")
BULK = ("y", "z")
LINE = ("core", "x")


def shifted(block, axis, distance):
    devices = range(lax.axis_size(axis))
    route = [(i - distance, i) for i in devices if i - distance in devices]
    return lax.ppermute(block, axis, route)


def swapped(block):
    return lax.ppermute(block, "core", [(0, 1), (1, 0)])


def exchanged(block, axis):
    return lax.all_to_all(block, axis, split_axis=0, concat_axis=0, tiled=True)


def product(left, right, dims=((1,), (0,))):
    return lax.dot_general(left, right, (dims, ((), ())), preferred_element_type=jnp.float32)


def written_ids(ids, columns):
    half = (ids.shape[0], columns // 2)
    high = jnp.broadcast_to((ids // RADIX)[:, None], half)
    low = jnp.broadcast_to((ids % RADIX)[:, None], half)
    return jnp.concatenate([high, low], axis=1).astype(jnp.bfloat16)


def read_ids(rows):
    middle = rows.shape[1] // 2
    pair = rows.astype(jnp.int32)
    return pair[:, :1] * RADIX + pair[:, middle : middle + 1]


def body(
    right_side,
    interface_inverse,
    face_link,
    far_target,
    far_rank,
    far_basis,
    patch_basis,
    corner_basis,
    corner_row,
    coarse_inverse,
):
    order = interface_inverse.shape[-1]
    columns = right_side.shape[-1]
    face_rows = order // 6
    inverse = interface_inverse.reshape(order, order)
    source = right_side.reshape(order, columns)
    links = face_link.reshape(4).astype(jnp.float32)
    rank_limit = far_basis.shape[-2]
    bases = far_basis.reshape(-1, order)
    patch = patch_basis.reshape(rank_limit, order)
    corners = corner_basis.reshape(-1, order)
    corner_count = corners.shape[0]
    ids = corner_row.reshape(-1)
    own_coarse, coarse_order = coarse_inverse.shape
    depth = lax.axis_size("z")
    bulk = lax.axis_size("y") * depth
    line = lax.axis_size("x")
    core = lax.axis_index("core")

    targets = far_target.reshape(-1, 1)
    ranks = far_rank.reshape(-1, 1)
    sides = jnp.bitwise_xor((targets // depth) % 2, core)
    places = sides * bulk + (targets // (2 * depth)) * depth + targets % depth
    row = jnp.arange(rank_limit, dtype=jnp.int32)[None, :]
    key = jnp.where(row < ranks, places * rank_limit + row, -1).reshape(1, -1)
    spots = 2 * bulk * rank_limit
    route = (jnp.arange(spots, dtype=jnp.int32)[:, None] == key).astype(jnp.bfloat16)

    id_rows = written_ids(ids, columns)
    line_ids = read_ids(
        exchanged(jnp.broadcast_to(id_rows[None], (line,) + id_rows.shape), "x").reshape(-1, columns)
    )
    local = line_ids - lax.axis_index("x") * own_coarse
    hot = (local == jnp.arange(own_coarse, dtype=jnp.int32)[None, :]).astype(jnp.bfloat16)
    held = product(hot, coarse_inverse).astype(jnp.bfloat16)
    spread = exchanged(jnp.broadcast_to(held[None], (line,) + held.shape), "x")
    own_rows = jnp.sum(spread.astype(jnp.float32), axis=0).astype(jnp.bfloat16)
    other_rows = swapped(own_rows)
    coarse_rows = jnp.where(
        core == 0,
        jnp.concatenate([own_rows, other_rows], axis=0),
        jnp.concatenate([other_rows, own_rows], axis=0),
    )

    multipliers = source.astype(jnp.float32)
    rounded = source
    coupling = None
    for sweep in range(ITERS):
        solved = product(inverse, rounded).astype(jnp.bfloat16)
        coefficient = product(bases, solved).astype(jnp.bfloat16)
        half = spots // 2
        outgoing = product(route[half:], coefficient).astype(jnp.bfloat16)
        incoming = swapped(outgoing)
        kept = product(route[:half], coefficient)
        far_rows = (kept + incoming.astype(jnp.float32)).astype(jnp.bfloat16)
        terms = product(corners, solved).astype(jnp.bfloat16)
        extra = terms if coupling is not None else jnp.concatenate([terms, id_rows], axis=0)
        payload = jnp.concatenate(
            [
                far_rows.reshape(bulk, rank_limit, columns),
                jnp.broadcast_to(extra[None], (bulk,) + extra.shape),
            ],
            axis=1,
        )
        landed = exchanged(payload, BULK)
        arrived = jnp.sum(landed[:, :rank_limit].astype(jnp.float32), axis=0).astype(jnp.bfloat16)
        last = rank_limit + corner_count
        all_terms = landed[:, rank_limit:last].reshape(-1, columns)
        if coupling is None:
            all_ids = read_ids(landed[:, last:].reshape(-1, columns))
            placed = (all_ids == jnp.arange(coarse_order, dtype=jnp.int32)[None, :]).astype(
                jnp.bfloat16
            )
            coupling = product(coarse_rows, placed, ((1,), (1,))).astype(jnp.bfloat16)
        partial = product(coupling, all_terms).astype(jnp.bfloat16)
        shares = exchanged(partial.reshape(-1, corner_count, columns), LINE)
        picked = jnp.sum(shares.astype(jnp.float32), axis=0).astype(jnp.bfloat16)

        pieces = []
        for offset, sent_face, axis in ((1, 1, GRID), (-1, 0, GRID), (1, 3, "x"), (-1, 2, "x")):
            sent = solved[sent_face * face_rows : (sent_face + 1) * face_rows]
            pieces.append(shifted(sent, axis, offset).astype(jnp.float32) * links[len(pieces)])
        pieces.append(jnp.zeros((order - 4 * face_rows, columns), jnp.float32))
        neighbour = jnp.concatenate(pieces, axis=0)
        far_term = product(patch, arrived, ((0,), (0,)))
        correction = product(corners, picked, ((0,), (0,)))
        multipliers = (
            multipliers
            + source.astype(jnp.float32)
            - (solved.astype(jnp.float32) - neighbour)
            - far_term
            - correction
        )
        rounded = multipliers.astype(jnp.bfloat16)
    field = product(inverse, rounded).astype(jnp.bfloat16)
    return multipliers.reshape(right_side.shape), field.reshape(right_side.shape)


def solution(mesh):
    sizes = mesh.shape
    fine = Mesh(
        mesh.devices.reshape(sizes["sx"] // 2, 2, sizes["sy"], sizes["sz"]), ("y", "core", "x", "z")
    )
    sub = P(GRID, "x", "z")
    return jax.shard_map(
        body,
        mesh=fine,
        in_specs=(sub,) * 9 + (P("x", None),),
        out_specs=(sub, sub),
        check_vma=False,
    )
```

```python
import functools

import jax
import jax.numpy as jnp
from jax import lax
from jax.experimental import pallas as pl
from jax.experimental.pallas import tpu as pltpu
from jax.sharding import Mesh
from jax.sharding import PartitionSpec as P

ITERS = 2
RADIX_BITS = 6
RADIX = 1 << RADIX_BITS
LANES = 128
GRID = ("y", "core")
BULK = ("y", "z")
LINE = ("core", "x")
SOLVE_PARTS = 3
FAR_PARTS = 2
LIMIT = 32 * 1024 * 1024

VMEM = pl.BlockSpec(memory_space=pltpu.VMEM)
HBM = pl.BlockSpec(memory_space=pltpu.HBM)
DMA = pltpu.SemaphoreType.DMA


def paired(block, axis, pairs):
    route = [(a, b) for a, b in pairs] + [(b, a) for a, b in pairs]
    return lax.ppermute(block, axis, route)


def turned(block, axis, distance):
    size = lax.axis_size(axis)
    return lax.ppermute(block, axis, [(i, (i + distance) % size) for i in range(size)])


def summed(block, axis):
    others = [turned(block, axis, distance) for distance in range(1, lax.axis_size(axis))]
    for other in others:
        block = block + other
    return block


def exchanged(block, axis):
    return lax.all_to_all(block, axis, split_axis=0, concat_axis=0, tiled=True)


def product(left, right, dims=((1,), (0,))):
    return lax.dot_general(left, right, (dims, ((), ())), preferred_element_type=jnp.float32)


def called(kernel, name, ins, outs, args, scratch=()):
    args = [
        pltpu.with_memory_space_constraint(arg, pltpu.HBM) if spec is HBM else arg
        for arg, spec in zip(args, ins)
    ]
    shapes = [pltpu.HBM(out.shape, out.dtype) if spec is HBM else out for out, spec in outs]
    return pl.pallas_call(
        kernel,
        out_shape=tuple(shapes),
        in_specs=ins,
        out_specs=tuple(spec for _, spec in outs),
        scratch_shapes=list(scratch),
        compiler_params=pltpu.CompilerParams(vmem_limit_bytes=LIMIT),
        name=name,
    )(*args)


def moved(source, target, sem):
    copy = pltpu.make_async_copy(source, target, sem)
    copy.start()
    return copy


def moved_parts(source, target, sems, parts):
    rows = source.shape[0] // parts
    copies = []
    for part in range(parts):
        where = pl.ds(part * rows, rows)
        copies.append(moved(source.at[where], target.at[where], sems.at[part]))
    return copies


def write_ids(ids_ref, slots_ref, rows_ref):
    count, columns = rows_ref.shape
    half = columns // 2
    sub = lax.broadcasted_iota(jnp.int32, (count, half), 0)
    high = jnp.zeros((count, half), jnp.int32)
    low = jnp.zeros((count, half), jnp.int32)
    for q in range(count):
        value = ids_ref[0, q]
        high = jnp.where(sub == q, value >> RADIX_BITS, high)
        low = jnp.where(sub == q, value & (RADIX - 1), low)
    rows = jnp.concatenate([high, low], axis=1).astype(jnp.float32).astype(jnp.bfloat16)
    rows_ref[...] = rows
    slots_ref[...] = jnp.zeros(slots_ref.shape, slots_ref.dtype)
    slots_ref[lax.axis_index("x")] = rows


def read_ids(rows):
    half = rows.shape[1] // 2
    return rows[:, :half] * float(RADIX) + rows[:, half:]


def hot_rows(ids, count, start):
    lane = lax.broadcasted_iota(jnp.int32, (1, LANES), 1).astype(jnp.float32)
    parts = []
    for block in range(count // LANES):
        local = ids - (start + float(block * LANES))
        parts.append((local == lane).astype(jnp.float32).astype(jnp.bfloat16))
    return jnp.concatenate(parts, axis=1)


def rows_kernel(slots_ref, coarse_ref, held_ref, coarse, sem):
    copy = moved(coarse_ref, coarse, sem)
    own = coarse_ref.shape[0]
    line, count, columns = slots_ref.shape
    rows = slots_ref[...].astype(jnp.float32).reshape(line * count, columns)
    start = (lax.axis_index("x") * own).astype(jnp.float32)
    hot = hot_rows(read_ids(rows), own, start)
    copy.wait()
    held_ref[...] = product(hot, coarse[...]).astype(jnp.bfloat16)


def routes(core, targets, ranks, route, shape):
    bulk, depth_bits, limit = shape
    entries = targets.shape[1]
    spots = entries * limit
    side = ((targets >> depth_bits) & 1) ^ core
    low = targets & ((1 << depth_bits) - 1)
    places = side * bulk + ((targets >> (depth_bits + 1)) << depth_bits) + low
    owner = lax.broadcasted_iota(jnp.int32, (entries, spots), 1) // limit
    entry = lax.broadcasted_iota(jnp.int32, (entries, spots), 0)
    widen = (owner == entry).astype(jnp.float32).astype(jnp.bfloat16)

    def spread(values):
        wide = jnp.broadcast_to(values.astype(jnp.float32), (limit, entries))
        return product(wide.astype(jnp.bfloat16), widen)

    row = lax.broadcasted_iota(jnp.int32, (limit, spots), 0).astype(jnp.float32)
    column = (lax.broadcasted_iota(jnp.int32, (limit, spots), 1) % limit).astype(jnp.float32)
    live = jnp.logical_and(row == column, row < spread(ranks))
    keys = jnp.where(live, spread(places), -1.0)
    for place in range(entries):
        hit = (keys == float(place)).astype(jnp.float32).astype(jnp.bfloat16)
        route[pl.ds(place * limit, limit), :] = hit


def corrected(base, corners, shares):
    picked = jnp.sum(shares.astype(jnp.float32), axis=0).astype(jnp.bfloat16)
    return base - product(corners, picked, ((0,), (0,)))


def solve_kernel(first, shape, *refs):
    targets_hbm, ranks_hbm, corners_hbm, inverse_hbm, bases_hbm = refs[:5]
    if first:
        source_hbm, ids_hbm, refs = refs[5], refs[6], refs[7:]
    else:
        base_hbm, shares_ref, refs = refs[5], refs[6], refs[7:]
    swap_ref, kept_ref, terms_ref, solved_hbm, grid_hbm, even_hbm, odd_hbm = refs[:7]
    refs = refs[7:]
    if first:
        slots_ref, id_rows_ref, refs = refs[0], refs[1], refs[2:]
    else:
        whole_hbm, refs = refs[0], refs[1:]
    targets, ranks, corners, inverse, bases, route, coefficient, solved_ref = refs[:8]
    sems, inverse_sems, bases_sems, refs = refs[8], refs[9], refs[10], refs[11:]
    core = lax.axis_index("core")
    odd = lax.axis_index("x") & 1
    face = grid_hbm.shape[0]
    half = kept_ref.shape[0]

    tables = [moved(targets_hbm, targets, sems.at[0]), moved(ranks_hbm, ranks, sems.at[1])]
    if first:
        source, ids = refs
        inputs = [moved(source_hbm, source, sems.at[2])]
        ids_copy = moved(ids_hbm, ids, sems.at[3])
    else:
        base, whole_ref = refs
        inputs = [moved(base_hbm, base, sems.at[2])]
    corner_copy = moved(corners_hbm, corners, sems.at[4])
    inverse_copies = moved_parts(inverse_hbm, inverse, inverse_sems, SOLVE_PARTS)
    bases_copies = moved_parts(bases_hbm, bases, bases_sems, FAR_PARTS)
    leaving = []
    for copy in tables:
        copy.wait()
    routes(core, targets[...], ranks[...], route, shape)
    if first:
        ids_copy.wait()
        write_ids(ids, slots_ref, id_rows_ref)
    corner_copy.wait()
    for copy in inputs:
        copy.wait()
    if first:
        rounded = source[...]
    else:
        whole = corrected(base[...], corners[...], shares_ref[...])
        whole_ref[...] = whole
        leaving.append(moved(whole_ref, whole_hbm, sems.at[5]))
        rounded = whole.astype(jnp.bfloat16)
    rows = inverse.shape[0] // SOLVE_PARTS
    for part, copy in enumerate(inverse_copies):
        copy.wait()
        where = pl.ds(part * rows, rows)
        solved_ref[where, :] = product(inverse[where, :], rounded).astype(jnp.bfloat16)
    leaving.append(moved(solved_ref, solved_hbm, sems.at[6]))

    def part_of(index):
        return solved_ref.at[pl.ds(pl.multiple_of(index * face, face), face)]

    leaving.append(moved(part_of(core), grid_hbm, sems.at[7]))
    leaving.append(moved(part_of(3 - odd), even_hbm, sems.at[8]))
    leaving.append(moved(part_of(2 + odd), odd_hbm, sems.at[9]))
    solved = solved_ref[...]
    rows = bases.shape[0] // FAR_PARTS
    for part, copy in enumerate(bases_copies):
        copy.wait()
        where = pl.ds(part * rows, rows)
        coefficient[where, :] = product(bases[where, :], solved).astype(jnp.bfloat16)
    terms_ref[...] = product(corners[...], solved).astype(jnp.bfloat16)
    values = coefficient[...]
    swap_ref[:half] = product(route[half:], values).astype(jnp.bfloat16)
    swap_ref[half:] = part_of(1 - core)[...]
    kept_ref[...] = product(route[:half], values)
    for copy in leaving:
        copy.wait()


def pack_kernel(count, *refs):
    kept_ref, swapped_ref, extras = refs[0], refs[1], refs[2:-3]
    payload_ref, face_hbm, sem = refs[-3:]
    bulk, _, columns = payload_ref.shape
    half = kept_ref.shape[0]
    copy = moved(swapped_ref.at[pl.ds(half, face_hbm.shape[0])], face_hbm, sem)
    total = kept_ref[...] + swapped_ref[:half].astype(jnp.float32)
    limit = half // bulk
    payload_ref[:, :limit] = total.reshape(bulk, limit, columns).astype(jnp.bfloat16)
    for number, extra in enumerate(extras):
        wide = jnp.broadcast_to(extra[...].astype(jnp.float32)[None], (bulk, count, columns))
        start = limit + number * count
        payload_ref[:, start : start + count] = wide.astype(jnp.bfloat16)
    copy.wait()


def middle_kernel(first, limit, count, *refs):
    if first:
        landed_ref, own_ref, other_ref, partial_ref, arrived_hbm, coupling_hbm = refs[:6]
        arrived_ref, coupling_ref, sems = refs[6:]
    else:
        landed_ref, coupling_ref, partial_ref, arrived_hbm, arrived_ref, sems = refs
    bulk, _, columns = landed_ref.shape

    def slab(number):
        start = limit + number * count
        block = landed_ref[:, start : start + count].astype(jnp.float32)
        return block.reshape(bulk * count, columns)

    terms = slab(0).astype(jnp.bfloat16)
    line = partial_ref.shape[0] // 2
    leaving = []
    if first:
        placed = hot_rows(read_ids(slab(1)), own_ref.shape[1], 0.0)
        for number, rows_ref in enumerate((own_ref, other_ref)):
            coupling = product(rows_ref[...], placed, ((1,), (1,)))
            coupling_ref[number] = coupling.astype(jnp.bfloat16)
        leaving.append(moved(coupling_ref, coupling_hbm, sems.at[0]))
    core = lax.axis_index("core")
    for number, start in enumerate((core * line, (1 - core) * line)):
        partial = product(coupling_ref[number], terms).reshape(line, count, columns)
        partial_ref[pl.ds(start, line)] = partial.astype(jnp.bfloat16)
    arrived = jnp.sum(landed_ref[:, :limit].astype(jnp.float32), axis=0)
    arrived_ref[...] = arrived.astype(jnp.bfloat16)
    leaving.append(moved(arrived_ref, arrived_hbm, sems.at[1]))
    for copy in leaving:
        copy.wait()


def update_kernel(*refs):
    count = (len(refs) - 6) // 2
    sources, (grid, even, odd_face), base_hbm = refs[:count], refs[count : count + 3], refs[count + 3]
    targets, (base_ref, sems) = refs[count + 4 : 2 * count + 4], refs[2 * count + 4 :]
    copies = [moved(a, b, sems.at[i]) for i, (a, b) in enumerate(zip(sources, targets))]
    for copy in copies:
        copy.wait()
    links, patch, arrived, source, whole, solved, swapped = targets
    core = lax.axis_index("core")
    odd = lax.axis_index("x") & 1
    face = grid.shape[0]
    far = product(patch[...], arrived[...], ((0,), (0,)))
    known = whole[...].astype(jnp.float32) + source[...].astype(jnp.float32)
    base_ref[...] = known - solved[...].astype(jnp.float32) - far
    for index, block in ((1 - core, swapped), (core, grid), (3 - odd, even), (2 + odd, odd_face)):
        where = pl.ds(pl.multiple_of(index * face, face), face)
        link = links[0, index].astype(jnp.float32)
        base_ref[where, :] = base_ref[where, :] + block[...].astype(jnp.float32) * link
    last = moved(base_ref, base_hbm, sems.at[count])
    last.wait()


def final_kernel(base_hbm, shares_ref, corners_hbm, inverse_hbm, whole_hbm, field_hbm, *scratch):
    base, corners, inverse, whole_ref, field_ref, sems, inverse_sems, field_sems = scratch
    inputs = [
        moved(base_hbm, base, sems.at[0]),
        moved(corners_hbm, corners, sems.at[2]),
    ]
    copies = moved_parts(inverse_hbm, inverse, inverse_sems, SOLVE_PARTS)
    for copy in inputs:
        copy.wait()
    whole = corrected(base[...], corners[...], shares_ref[...])
    whole_ref[...] = whole
    leaving = [moved(whole_ref, whole_hbm, sems.at[3])]
    rounded = whole.astype(jnp.bfloat16)
    rows = inverse.shape[0] // SOLVE_PARTS
    for part, copy in enumerate(copies):
        copy.wait()
        where = pl.ds(part * rows, rows)
        field_ref[where, :] = product(inverse[where, :], rounded).astype(jnp.bfloat16)
        leaving.append(moved(field_ref.at[where], field_hbm.at[where], field_sems.at[part]))
    for copy in leaving:
        copy.wait()


def body(
    right_side,
    interface_inverse,
    face_link,
    far_target,
    far_rank,
    far_basis,
    patch_basis,
    corner_basis,
    corner_row,
    coarse_inverse,
):
    bf16, f32, i32 = jnp.bfloat16, jnp.float32, jnp.int32
    order = interface_inverse.shape[-1]
    columns = right_side.shape[-1]
    face = order // 6
    inverse = interface_inverse.reshape(order, order)
    source = right_side.reshape(order, columns)
    links = face_link.reshape(1, -1)
    limit = far_basis.shape[-2]
    bases = far_basis.reshape(-1, order)
    patch = patch_basis.reshape(limit, order)
    corners = corner_basis.reshape(-1, order)
    count = corners.shape[0]
    ids = corner_row.reshape(1, -1)
    own_coarse, coarse_order = coarse_inverse.shape
    targets = far_target.reshape(1, -1)
    ranks = far_rank.reshape(1, -1)
    entries = targets.shape[1]
    depth = lax.axis_size("z")
    bulk = lax.axis_size("y") * depth
    line = lax.axis_size("x")
    spots = bases.shape[0]
    half = spots // 2
    shape = (bulk, depth.bit_length() - 1, limit)
    struct = jax.ShapeDtypeStruct
    near = [(i, i + 1) for i in range(0, line, 2)]
    apart = [(i, i + 1) for i in range(1, line - 1, 2)]
    between = [(i, i + 1) for i in range(1, 2 * lax.axis_size("y") - 1, 2)]

    whole = source
    base = shares = coupling = None
    for sweep in range(ITERS):
        initial = sweep == 0
        outs = [
            (struct((half + face, columns), bf16), VMEM),
            (struct((half, columns), f32), VMEM),
            (struct((count, columns), bf16), VMEM),
            (struct((order, columns), bf16), HBM),
        ] + [(struct((face, columns), bf16), HBM)] * 3
        args = [targets, ranks, corners, inverse, bases]
        scratch = [
            pltpu.VMEM((1, entries), i32),
            pltpu.VMEM((1, entries), i32),
            pltpu.VMEM((count, order), bf16),
            pltpu.VMEM((order, order), bf16),
            pltpu.VMEM((spots, order), bf16),
            pltpu.VMEM((spots, spots), bf16),
            pltpu.VMEM((spots, columns), bf16),
            pltpu.VMEM((order, columns), bf16),
            DMA((10,)),
            DMA((SOLVE_PARTS,)),
            DMA((FAR_PARTS,)),
        ]
        if initial:
            args += [source, ids]
            outs += [
                (struct((line, count, columns), bf16), VMEM),
                (struct((count, columns), bf16), VMEM),
            ]
            scratch += [pltpu.VMEM((order, columns), bf16), pltpu.SMEM((1, count), i32)]
        else:
            args += [base, shares]
            outs += [(struct((order, columns), f32), HBM)]
            scratch += [pltpu.VMEM((order, columns), f32)] * 2
        results = called(
            functools.partial(solve_kernel, initial, shape),
            "solve",
            [HBM] * 6 + [HBM if initial else VMEM],
            outs,
            args,
            scratch,
        )
        swap, kept, terms, solved, to_grid, to_even, to_odd = results[:7]
        extras = [terms]
        if initial:
            slots, id_rows = results[7:]
            extras += [id_rows]
            slots = summed(slots, "x")
        else:
            whole = results[7]
        swapped = paired(swap, "core", [(0, 1)])
        payload, from_core = called(
            functools.partial(pack_kernel, count),
            "pack",
            [VMEM] * (2 + len(extras)),
            [
                (struct((bulk, limit + count * len(extras), columns), bf16), VMEM),
                (struct((face, columns), bf16), HBM),
            ],
            [kept, swapped] + extras,
            [DMA],
        )
        landed = exchanged(payload, BULK)
        if initial:
            (held,) = called(
                rows_kernel,
                "rows",
                [VMEM, HBM],
                [(struct((line * count, coarse_order), bf16), VMEM)],
                (slots, coarse_inverse),
                [pltpu.VMEM((own_coarse, coarse_order), bf16), DMA],
            )
            own_rows = summed(held, "x")
            other_rows = paired(own_rows, "core", [(0, 1)])
        from_grid = paired(to_grid, GRID, between)
        from_even = paired(to_even, "x", near)
        from_odd = paired(to_odd, "x", apart)
        args = [landed] + ([own_rows, other_rows] if initial else [coupling])
        outs = [
            (struct((2 * line, count, columns), bf16), VMEM),
            (struct((limit, columns), bf16), HBM),
        ]
        scratch = [pltpu.VMEM((limit, columns), bf16)]
        if initial:
            outs += [(struct((2, line * count, bulk * count), bf16), HBM)]
            scratch += [pltpu.VMEM((2, line * count, bulk * count), bf16)]
        results = called(
            functools.partial(middle_kernel, initial, limit, count),
            "middle",
            [VMEM] * len(args),
            outs,
            args,
            scratch + [DMA((2,))],
        )
        partial, arrived = results[:2]
        if initial:
            coupling = results[2]
        shares = exchanged(partial, LINE)
        args = [links, patch, arrived, source, whole, solved, from_core]
        (base,) = called(
            update_kernel,
            "update",
            [HBM] * len(args) + [VMEM] * 3,
            [(struct((order, columns), f32), HBM)],
            args + [from_grid, from_even, from_odd],
            [pltpu.SMEM(links.shape, i32)]
            + [pltpu.VMEM(arg.shape, arg.dtype) for arg in args[1:]]
            + [pltpu.VMEM((order, columns), f32), DMA((len(args) + 1,))],
        )
    whole, field = called(
        final_kernel,
        "final",
        [HBM, VMEM, HBM, HBM],
        [(struct((order, columns), f32), HBM), (struct((order, columns), bf16), HBM)],
        (base, shares, corners, inverse),
        [
            pltpu.VMEM((order, columns), f32),
            pltpu.VMEM((count, order), bf16),
            pltpu.VMEM((order, order), bf16),
            pltpu.VMEM((order, columns), f32),
            pltpu.VMEM((order, columns), bf16),
            DMA((4,)),
            DMA((SOLVE_PARTS,)),
            DMA((SOLVE_PARTS,)),
        ],
    )
    return whole.reshape(right_side.shape), field.reshape(right_side.shape)


def solution(mesh):
    sizes = mesh.shape
    fine = Mesh(
        mesh.devices.reshape(sizes["sx"] // 2, 2, sizes["sy"], sizes["sz"]), ("y", "core", "x", "z")
    )
    sub = P(GRID, "x", "z")
    return jax.shard_map(
        body,
        mesh=fine,
        in_specs=(sub,) * 9 + (P("x", None),),
        out_specs=(sub, sub),
        check_vma=False,
    )
```
